128 devices in a mesh: dp: 4 (over x), expert: 32 (over z, y, core).
Axes of the slice: x: 4, y: 4, z: 4, core: 2. Of those that a mesh axis runs over, the one named last changes fastest.
Arguments:
- tokens: bfloat16 [2, 8192, 4096], P(None, ('dp', 'expert')), may hold values from -64 to 64
- expert_of: int32 [2, 8192], P(None, ('dp', 'expert')), may hold values from 0 to 15, as said below
- w_gate: bfloat16 [32, 4096, 3584], P('expert', None, 'dp'), may hold values from -0.09375 to 0.09375
- w_up: bfloat16 [32, 4096, 3584], P('expert', None, 'dp'), may hold values from -0.09375 to 0.09375
- w_down: bfloat16 [32, 3584, 4096], P('expert', 'dp'), may hold values from -1 to 1
Outputs:
- out: bfloat16 [2, 8192, 4096], P(None, ('dp', 'expert'))
- next_scale: float32 [16], replicated
The draws below stay inside these ranges and needn't reach their ends.
Inputs may be any that keep to these rules, and one draw needn't show every extreme that they name: `expert_of`: in each microbatch the 64 tokens of one device name each expert at most 4 times, and one expert, the same for all devices of that microbatch, exactly 4 times.
All inputs are finite; a program needn't handle non-finite values.
Results may differ from the reference program's by a relative error of at most 0.012.
Values may be sent and summed in bfloat16 or wider, within the bound.
No kernel may reach another device: no remote copies, remote signals or barrier semaphores. Data moves between devices by JAX's collectives and lax.ppermute only.
A program may use at most 128 MiB of HBM per device.

```python
import math
import jax
import jax.numpy as jnp
from jax import lax

D = 4096
FF = 7168
SPAN = 2
MICRO = 2
TOK_DEV = 64
EXPERTS = 16
CAP = 4
TOKENS = 8192
N_DP = 4


def draw_tokens(key, part):
    keys_all = jax.random.split(jax.random.fold_in(key, 3), 4)
    shape_all = (MICRO, TOKENS, D)
    base_values = jnp.clip(jax.random.normal(keys_all[0], shape_all, jnp.float32), -5.5, 5.5)
    row_scale = jnp.exp(jax.random.uniform(keys_all[2], (MICRO, TOKENS, 1), jnp.float32, math.log(0.2), math.log(2.0)))
    rising = jnp.exp(0.5 * math.log(3.0) * jnp.arange(TOKENS, dtype=jnp.float32) / max(TOKENS - 1, 1))[None, :, None]
    column_scale = jnp.exp(jax.random.uniform(keys_all[3], (1, 1, D), jnp.float32, math.log(0.32), math.log(3.2)))
    return (base_values * row_scale * rising * column_scale).astype(jnp.bfloat16)


def draw_w_down(key, part):
    keys_all = jax.random.split(jax.random.fold_in(key, 5), 2)
    shape_all = (EXPERTS, SPAN, FF // SPAN, D)
    base_values = jnp.clip(jax.random.normal(keys_all[0], shape_all, jnp.float32), -6.0, 6.0)
    ladder = jnp.arange(EXPERTS, dtype=jnp.float32) / max(EXPERTS - 1, 1)
    gain_ladder = jnp.exp(math.log(0.25) + ladder * (math.log(2.5) - math.log(0.25)))
    expert_gain = jax.random.permutation(keys_all[1], gain_ladder).reshape(EXPERTS, 1, 1, 1)
    weights = base_values * expert_gain * FF ** (-0.5)
    return weights.reshape(EXPERTS * SPAN, FF // SPAN, D).astype(jnp.bfloat16)


def draw_expert_of(key, part):
    blocks = TOKENS // TOK_DEV

    def one_block(block_key, full_expert):
        first_key, second_key = jax.random.split(block_key)
        others = jnp.arange(EXPERTS - 1, dtype=jnp.int32)
        others = jnp.where(others >= full_expert, others + 1, others).astype(jnp.int32)
        slot_pool = jnp.repeat(others, CAP)
        chosen = jax.random.permutation(first_key, slot_pool)[:TOK_DEV - CAP]
        block_ids = jnp.concatenate([jnp.full((CAP,), full_expert, jnp.int32), chosen.astype(jnp.int32)])
        return jax.random.permutation(second_key, block_ids)

    def one_micro(micro_key):
        full_key, block_key = jax.random.split(micro_key)
        full_expert = jax.random.randint(full_key, (), 0, EXPERTS, dtype=jnp.int32)
        block_keys = jax.random.split(block_key, blocks)
        return jax.vmap(lambda single_key: one_block(single_key, full_expert))(block_keys)
    micro_keys = jax.random.split(jax.random.fold_in(key, 11), MICRO)
    return jax.vmap(one_micro)(micro_keys).reshape(MICRO, TOKENS).astype(jnp.int32)


def block_scale(rng, extent, cuts, least, largest):
    factor_of = 1.0
    for axis_at, blocks in cuts:
        heights = jax.random.uniform(jax.random.fold_in(jax.random.fold_in(rng, 6), axis_at), (blocks,), jnp.float32, least / len(cuts), largest / len(cuts))
        factor_of = factor_of * jnp.repeat(jnp.exp(heights), extent[axis_at] // blocks).reshape((-1,) + (1,) * (len(extent) - 1 - axis_at))
    return factor_of


def scatter_about(own_key, shape, deviation, bound, cuts=(), held_as=jnp.bfloat16):
    entries = deviation * jax.random.normal(own_key, shape, jnp.float32)
    if cuts:
        entries = entries * block_scale(own_key, shape, cuts, -0.22, 0.18)
    return jnp.clip(entries, -bound, bound).astype(held_as)


def setup_inputs(seed: int = 0) -> dict:
    arg_keys = jax.random.split(jax.random.key(seed), 6)
    return {
        "tokens": draw_tokens(jax.random.fold_in(arg_keys[5], 71), 0),
        "expert_of": draw_expert_of(jax.random.fold_in(arg_keys[5], 71), 0),
        "w_gate": scatter_about(arg_keys[2], (EXPERTS * SPAN, D, FF // SPAN), D ** -0.5, 0.09375, ((0, 32), (2, 4))),
        "w_up": scatter_about(arg_keys[3], (EXPERTS * SPAN, D, FF // SPAN), D ** -0.5, 0.09375, ((0, 32), (2, 4))),
        "w_down": draw_w_down(jax.random.fold_in(arg_keys[5], 71), 0),
    }


clip_target = 2.0

def block_slots(block_ids):
    onehot_ids = (block_ids[:, None] == jnp.arange(EXPERTS, dtype=jnp.int32)[None, :]).astype(jnp.int32)
    earlier = jnp.cumsum(onehot_ids, axis=0) - onehot_ids
    return lax.optimization_barrier(jnp.sum(earlier * onehot_ids, axis=1)).astype(jnp.int32)

def expert_rows(operands):
    rows_in, gate_rows, up_rows, down_rows = operands
    group_width = FF // (SPAN * N_DP)
    total_out = jnp.zeros((rows_in.shape[0], D), jnp.float32)
    for half_idx in range(SPAN):
        summed = jnp.zeros((rows_in.shape[0], D), jnp.float32)
        for quarter in range(N_DP):
            low_col = quarter * group_width
            gate_vals = jnp.dot(rows_in, gate_rows[half_idx, :, low_col:low_col + group_width], preferred_element_type=jnp.float32)
            up_vals = jnp.dot(rows_in, up_rows[half_idx, :, low_col:low_col + group_width], preferred_element_type=jnp.float32)
            hidden = (jax.nn.silu(gate_vals) * up_vals).astype(jnp.bfloat16)
            part_out = jnp.dot(hidden, down_rows[half_idx, low_col:low_col + group_width, :], preferred_element_type=jnp.float32)
            part_out = lax.optimization_barrier(part_out.astype(jnp.bfloat16))
            summed = summed + part_out.astype(jnp.float32)
        half_out = lax.optimization_barrier(summed.astype(jnp.bfloat16))
        total_out = total_out + half_out.astype(jnp.float32)
    return total_out

def reference(tokens, expert_of, w_gate, w_up, w_down):
    blocks = TOKENS // TOK_DEV
    gate_all = w_gate.reshape(EXPERTS, SPAN, D, FF // SPAN)
    up_all = w_up.reshape(EXPERTS, SPAN, D, FF // SPAN)
    down_all = w_down.reshape(EXPERTS, SPAN, FF // SPAN, D)
    clip_scale = jnp.ones((EXPERTS,), jnp.float32)
    outputs = []
    for micro_idx in range(MICRO):
        token_ids = expert_of[micro_idx].astype(jnp.int32)
        slot_of = jax.vmap(block_slots)(token_ids.reshape(blocks, TOK_DEV)).reshape(TOKENS)
        block_of = (jnp.arange(TOKENS, dtype=jnp.int32) // TOK_DEV).astype(jnp.int32)
        gated = (clip_scale[token_ids][:, None] * tokens[micro_idx].astype(jnp.float32)).astype(jnp.bfloat16)
        position = ((token_ids * blocks + block_of) * CAP + slot_of).astype(jnp.int32)
        dispatched = jnp.zeros((EXPERTS * blocks * CAP, D), jnp.bfloat16).at[position].set(gated)
        dispatched = dispatched.reshape(EXPERTS, blocks * CAP, D)
        expert_out = lax.map(expert_rows, (dispatched, gate_all, up_all, down_all))
        token_out = expert_out.reshape(EXPERTS * blocks * CAP, D)[position]
        outputs.append(token_out.astype(jnp.bfloat16))
        squares = lax.optimization_barrier(jnp.sum(token_out * token_out, axis=1))
        counts = jax.ops.segment_sum(jnp.ones((TOKENS,), jnp.float32), token_ids, EXPERTS)
        square_sums = jax.ops.segment_sum(squares, token_ids, EXPERTS)
        clip_scale = jnp.minimum(1.0, clip_target / jnp.sqrt((square_sums + D) / (D * (counts + 1.0))))
    return (jnp.stack(outputs), clip_scale)
```

```python
import functools

import jax
import jax.numpy as jnp
from jax import lax
from jax.experimental import pallas as pl
from jax.experimental.pallas import tpu as pltpu
from jax.sharding import Mesh
from jax.sharding import PartitionSpec as P

X = "dp"
PLANE = ("expert_0", "expert_1")
CORE = "expert_2"
EXPERT = ("expert_0", "expert_1", "expert_2")
DP_EXPERT = ("dp", "expert_0", "expert_1", "expert_2")
STAT = 128
MIB = 1 << 20

clip_target = 2.0


WHOLE = pl.BlockSpec(memory_space=pltpu.VMEM)
SCALAR = pl.BlockSpec(memory_space=pltpu.SMEM)
HBM = pl.BlockSpec(memory_space=pltpu.HBM)
f32 = jnp.float32
bf16 = jnp.bfloat16


def along_x(v, sign):
    n = lax.axis_size(X)
    pairs = []
    for i in range(n):
        pairs.append((2 * i, 2 * ((i + sign) % n)))
        pairs.append((2 * i + 1, 2 * ((i - sign) % n) + 1))
    return lax.ppermute(v, (X, CORE), pairs)


def swap_core(v):
    return lax.ppermute(v, CORE, [(0, 1), (1, 0)])


def line_sum(v):
    v = v + swap_core(v)
    v = v + lax.ppermute(v, X, [(0, 1), (1, 0), (2, 3), (3, 2)])
    return v + lax.ppermute(v, X, [(0, 3), (3, 0), (1, 2), (2, 1)])


def call(kernel, out_shape, limit, *args, scratch=(), specs=None):
    return pl.pallas_call(
        kernel,
        in_specs=specs or [WHOLE] * len(args),
        out_specs=[WHOLE] * len(out_shape),
        out_shape=out_shape,
        scratch_shapes=list(scratch),
        compiler_params=pltpu.CompilerParams(vmem_limit_bytes=limit),
    )(*args)


def shape_of(*dims, dtype=bf16):
    return jax.ShapeDtypeStruct(dims, dtype)


def load_kernel(*refs):
    n = len(refs) // 2
    sems = refs[-1]
    copies = [pltpu.make_async_copy(refs[i], refs[n + i], sems.at[i]) for i in range(n)]
    for c in copies:
        c.start()
    for c in copies:
        c.wait()


def load(*weights):
    weights = [pltpu.with_memory_space_constraint(w, pltpu.HBM) for w in weights]
    return call(
        load_kernel,
        [pltpu.VMEM(w.shape, w.dtype) for w in weights],
        2 * MIB,
        *weights,
        specs=[HBM] * len(weights),
        scratch=[pltpu.SemaphoreType.DMA((len(weights),))],
    )


OVER_ROWS = (((0,), (0,)), ((), ()))


def pick(rows, cols, which, target):
    s = lax.broadcasted_iota(jnp.int32, (rows, cols), 0)
    slot = (s // 8) * 4 + s % 4
    hit = jnp.where((s // 4) % 2 == which, slot, -1) == target
    return jnp.where(hit, 1.0, 0.0).astype(bf16)


def positions(ids, experts):
    n = ids.shape[1]
    onehot = jnp.where(lax.broadcasted_iota(jnp.int32, (experts, n), 0) == ids, 1.0, 0.0)
    row = lax.broadcasted_iota(jnp.int32, (n, n), 0)
    col = lax.broadcasted_iota(jnp.int32, (n, n), 1)
    before = jnp.where(row < col, 1.0, 0.0).astype(bf16)
    earlier = jnp.dot(onehot.astype(bf16), before, preferred_element_type=f32)
    slot = jnp.sum(earlier * onehot, axis=0, keepdims=True).astype(jnp.int32)
    return ids * (n // experts) + slot


def pack_kernel(tokens, ids, sending, *, experts):
    micros, n, width = tokens.shape
    places = [pick(2 * n, n, m, positions(ids[m : m + 1, :], experts)) for m in range(micros)]
    for lo in range(0, width, 1024):
        at = slice(lo, lo + 1024)
        out = jnp.dot(places[0], tokens[0, :, at], preferred_element_type=f32)
        out = out + jnp.dot(places[1], tokens[1, :, at], preferred_element_type=f32)
        sending[:, at] = out.astype(bf16)
    ones = jnp.ones((n, STAT), bf16)
    fill = jnp.dot(places[0], ones, preferred_element_type=f32)
    fill = fill + jnp.dot(places[1], ones, preferred_element_type=f32)
    sending[:, width:] = fill.astype(bf16)


def pack(tokens, ids, experts):
    micros, n, width = tokens.shape
    return call(
        functools.partial(pack_kernel, experts=experts),
        [shape_of(micros * n, width + STAT)],
        8 * MIB,
        tokens,
        ids,
    )[0]


def split_kernel(arrived, *outs):
    *mine, counts = outs
    n, width = mine[0].shape
    rows = arrived.shape[0]
    for m, out in enumerate(mine):
        take = pick(rows, n, m, lax.broadcasted_iota(jnp.int32, (rows, n), 1))
        for lo in range(0, width, 1024):
            at = slice(lo, lo + 1024)
            out[:, at] = lax.dot_general(
                take, arrived[:, at], OVER_ROWS, preferred_element_type=f32
            ).astype(bf16)
    fill = arrived[:, width:].astype(f32)
    s = lax.broadcasted_iota(jnp.int32, fill.shape, 0)
    for m in range(len(mine)):
        count = jnp.sum(jnp.where((s // 4) % 2 == m, fill, 0.0), axis=0, keepdims=True)
        counts[m * 8 : m * 8 + 8, :] = jnp.broadcast_to(count, (8, STAT))


def split(arrived, micros, width):
    n = arrived.shape[0] // micros
    *mine, counts = call(
        split_kernel,
        [shape_of(n, width)] * micros + [shape_of(8 * micros, STAT, dtype=f32)],
        8 * MIB,
        arrived,
    )
    return mine, counts


def silu_mul(g, u):
    return (g / (1.0 + jnp.exp(-g)) * u).astype(bf16)


def gate_up_kernel(*refs, groups, keep):
    parts = refs[:groups]
    wg, wu = refs[groups : groups + 2]
    outs = refs[groups + 2 : -1]
    x = refs[-1]
    rows = parts[0].shape[0]
    for i, part in enumerate(parts):
        x[i * rows : (i + 1) * rows, :] = part[...]
    tile = 128

    def step(i, carry):
        at = pl.ds(pl.multiple_of(i * tile, tile), tile)
        w = jnp.concatenate([wg[0, :, at], wu[0, :, at]], axis=1)
        both = jnp.dot(x[...], w, preferred_element_type=f32)
        g = both[:, :tile]
        u = both[:, tile:]
        if keep:
            outs[0][:, at] = g
            outs[1][:, at] = u
        else:
            outs[0][:, at] = silu_mul(g, u)
        return carry

    lax.fori_loop(0, wg.shape[2] // tile, step, 0)


def gate_up(parts, w_gate, w_up, keep):
    rows, k = parts[0].shape
    dims = (len(parts) * rows, w_gate.shape[2])
    return call(
        functools.partial(gate_up_kernel, groups=len(parts), keep=keep),
        [shape_of(*dims, dtype=f32)] * 2 if keep else [shape_of(*dims)],
        14 * MIB,
        *parts,
        w_gate,
        w_up,
        scratch=[pltpu.VMEM((dims[0], k), bf16)],
    )


def down_kernel(*refs, groups, keep):
    if keep:
        clip = refs[0][0, 0]
        parts = refs[1 : 1 + 2 * groups]
        sizes = [parts[2 * i].shape[0] // 2 for i in range(groups)]
    else:
        parts = refs[:groups]
        sizes = [p.shape[0] // 2 for p in parts]
    w, *owns, oth, h = refs[int(keep) + len(parts) :]
    n = owns[0].shape[0]
    rows = oth.shape[0]
    at = 0
    for i, size in enumerate(sizes):
        for side in range(2):
            src = slice(side * size, (side + 1) * size)
            dst = slice(side * rows + at, side * rows + at + size)
            if keep:
                h[dst, :] = silu_mul(clip * parts[2 * i][src, :], clip * parts[2 * i + 1][src, :])
            else:
                h[dst, :] = parts[i][src, :]
        at += size
    tile = 512

    def step(i, carry):
        cols = pl.ds(pl.multiple_of(i * tile, tile), tile)
        y = jnp.dot(h[...], w[0, :, cols], preferred_element_type=f32)
        for j, own in enumerate(owns):
            own[:, cols] = y[j * n : (j + 1) * n]
        oth[:, cols] = y[rows:].astype(oth.dtype)
        return carry

    lax.fori_loop(0, w.shape[2] // tile, step, 0)


def down(groups, w_down, n, clip):
    keep = clip is not None
    rows = sum(g[0].shape[0] for g in groups) // 2
    k, width = w_down.shape[1:]
    args = [a for g in groups for a in g]
    specs = [WHOLE] * (len(args) + 1)
    if keep:
        args = [clip] + args
        specs = [SCALAR] + specs
    return call(
        functools.partial(down_kernel, groups=len(groups), keep=keep),
        [shape_of(n, width, dtype=f32)] * (rows // n) + [shape_of(rows, width)],
        12 * MIB,
        *args,
        w_down,
        scratch=[pltpu.VMEM((2 * rows, k), bf16)],
        specs=specs,
    )


def finish_kernel(own, other, near_a, near_b, counts, *outs, micro, last):
    n, width = own.shape
    half = width // 2
    tile = 512
    rows = 2 * n
    places = [pick(rows, n, h, lax.broadcasted_iota(jnp.int32, (rows, n), 1)) for h in range(2)]

    def step(i, total):
        out = None
        for h in range(2):
            cols = pl.ds(pl.multiple_of(h * half + i * tile, tile), tile)
            fin = own[:, cols] + other[:n, cols].astype(f32)
            fin = fin + (near_a[:, cols].astype(f32) + near_b[:, cols].astype(f32))
            part = jnp.dot(places[h], fin.astype(bf16), preferred_element_type=f32)
            out = part if out is None else out + part
            sq = fin * fin
            for j in range(0, tile, STAT):
                total = total + sq[:, j : j + STAT]
        outs[0][:, pl.ds(pl.multiple_of(i * tile, tile), tile)] = out.astype(bf16)
        return total

    total = lax.fori_loop(0, half // tile, step, jnp.zeros((n, STAT), f32))
    total = jnp.sum(jnp.sum(total, axis=0, keepdims=True), axis=1, keepdims=True)
    count = counts[micro * 8 : micro * 8 + 1, :1]
    if last:
        total = jnp.broadcast_to(total, (rows, STAT))
        lane = lax.broadcasted_iota(jnp.int32, (rows, STAT), 1)
        high = total.astype(bf16).astype(f32)
        middle = (total - high).astype(bf16).astype(f32)
        low = total - high - middle
        stats = jnp.where(lane == 0, high, jnp.where(lane == 1, middle, low))
        stats = jnp.where(lane < 3, stats, jnp.where(lane == 3, count, 0.0))
        outs[0][:, half:] = stats.astype(bf16)
    else:
        lane = lax.broadcasted_iota(jnp.int32, (8, STAT), 1)
        total = jnp.broadcast_to(total, (8, STAT))
        outs[1][...] = jnp.where(lane == 0, total, jnp.where(lane == 1, count, 0.0))


def finish(own, other, near_a, near_b, counts, micro, last):
    n, width = own.shape
    half = width // 2
    if last:
        outs = [shape_of(2 * n, half + STAT)]
    else:
        outs = [shape_of(2 * n, half), shape_of(8, STAT, dtype=f32)]
    return call(
        functools.partial(finish_kernel, micro=micro, last=last),
        outs,
        10 * MIB,
        own,
        other,
        near_a,
        near_b,
        counts,
    )


def unpack_kernel(*refs, experts):
    *backs, ids, out = refs
    n, width = out.shape[1:]
    half = width // 2
    for m, back in enumerate(backs):
        position = positions(ids[m : m + 1, :], experts)
        for h in range(2):
            take = pick(2 * n, n, h, position)
            for lo in range(0, half, 1024):
                out[m, :, h * half + lo : h * half + lo + 1024] = lax.dot_general(
                    take, back[:, lo : lo + 1024], OVER_ROWS, preferred_element_type=f32
                ).astype(bf16)


def exchange(v):
    experts = lax.axis_size(PLANE)
    rows, width = v.shape
    out = lax.all_to_all(v.reshape(experts, rows // experts, width), PLANE, 0, 0, tiled=True)
    return out.reshape(rows, width)


def body(tokens, expert_of, w_gate, w_up, w_down):
    micros, n, width = tokens.shape
    experts = lax.axis_size(PLANE)
    tie = lax.optimization_barrier

    def clip_of(sumsq, count):
        return jnp.minimum(
            1.0, clip_target / jnp.sqrt((sumsq + width) / (width * (count + 1.0)))
        )

    arrived = exchange(pack(tokens, expert_of, experts))
    mine, counts = split(arrived, micros, width)
    w_gate, w_up, w_down = load(w_gate, w_up, w_down)

    def spread_near(m):
        a = along_x(mine[m], 1)
        b = along_x(mine[m], -1)
        o = swap_core(mine[m])
        own = gate_up([mine[m], o], w_gate, w_up, m > 0)
        return a, b, own

    def spread_far(m, a, b):
        far = along_x(a, 1)
        ao = swap_core(a)
        bo = swap_core(b)
        near = gate_up([a, b, ao, bo], w_gate, w_up, m > 0)
        return far, near

    def spread_last(m, far):
        return gate_up([far, swap_core(far)], w_gate, w_up, m > 0)

    def collect(m, own, near, far, clip, fill_in):
        mid, send_far = down([far], w_down, n, clip)
        mid = mid + swap_core(send_far).astype(f32)
        relay = along_x(mid.astype(bf16), 1)
        mine_o, a_o, b_o, send = down([own, near], w_down, n, clip)
        got = swap_core(send)
        to_a = (a_o + got[n : 2 * n].astype(f32)).astype(bf16)
        from_b = along_x(to_a, -1)
        got_b, relay = tie((got, relay))
        to_b = (b_o + got_b[2 * n :].astype(f32) + relay.astype(f32)).astype(bf16)
        from_a = along_x(to_b, 1)
        from_a, from_b, extra = fill_in(from_a, from_b)
        last = m + 1 == micros
        return finish(mine_o, got, from_a, from_b, counts, m, last), extra

    a0, b0, own0 = spread_near(0)
    far0, near0 = spread_far(0, a0, b0)
    mine[1], near0 = tie((mine[1], near0))
    a1, b1, own1 = spread_near(1)
    far0 = spread_last(0, far0)

    def gates_of_1(from_a, from_b):
        ao = swap_core(a1)
        bo = swap_core(b1)
        near1 = gate_up([a1, b1, ao, bo], w_gate, w_up, True)
        from_a, from_b, near1, a = tie((from_a, from_b, near1, a1))
        far1 = along_x(a, 1)
        return from_a, from_b, (near1, far1)

    (out0, stats), (near1, far1) = collect(0, own0, near0, far0, None, gates_of_1)
    stats = line_sum(stats)
    far1 = spread_last(1, far1)
    clip = clip_of(stats[:1, :1], stats[:1, 1:2])

    def return_0(from_a, from_b):
        back = exchange(out0)
        from_a, from_b, back = tie((from_a, from_b, back))
        return from_a, from_b, back

    (out1,), back0 = collect(1, own1, near1, far1, clip, return_0)
    back1 = exchange(out1)
    got = line_sum(back1[:: 2 * n // experts, width // 2 :].astype(f32))
    scale = clip_of(got[:, 0] + got[:, 1] + got[:, 2], got[:, 3])
    (out,) = call(
        functools.partial(unpack_kernel, experts=experts),
        [shape_of(micros, n, width)],
        8 * MIB,
        back0,
        back1[:, : width // 2],
        expert_of,
    )
    return out, scale


def solution(mesh):
    finer = Mesh(
        mesh.devices.reshape(mesh.shape["dp"], 4, 4, 2), ("dp", "expert_0", "expert_1", "expert_2")
    )
    placed = (
        P(None, DP_EXPERT, None),
        P(None, DP_EXPERT),
        P(EXPERT, None, "dp"),
        P(EXPERT, None, "dp"),
        P(EXPERT, "dp", None),
    )
    return jax.shard_map(
        body,
        mesh=finer,
        in_specs=placed,
        out_specs=(P(None, DP_EXPERT, None), P()),
        check_vma=False,
    )
```

```python
import functools

import jax
import jax.numpy as jnp
from jax import lax
from jax.experimental import pallas as pl
from jax.experimental.pallas import tpu as pltpu
from jax.sharding import Mesh
from jax.sharding import PartitionSpec as P

X = "dp"
PLANE = ("expert_0", "expert_1")
CORE = "expert_2"
EXPERT = ("expert_0", "expert_1", "expert_2")
DP_EXPERT = ("dp", "expert_0", "expert_1", "expert_2")
STAT = 128
MIB = 1 << 20

clip_target = 2.0


WHOLE = pl.BlockSpec(memory_space=pltpu.VMEM)
HBM = pl.BlockSpec(memory_space=pltpu.HBM)
f32 = jnp.float32
bf16 = jnp.bfloat16


def along_x(v, sign):
    n = lax.axis_size(X)
    pairs = []
    for i in range(n):
        pairs.append((2 * i, 2 * ((i + sign) % n)))
        pairs.append((2 * i + 1, 2 * ((i - sign) % n) + 1))
    return lax.ppermute(v, (X, CORE), pairs)


def swap_core(v):
    return lax.ppermute(v, CORE, [(0, 1), (1, 0)])


def line_sum(v):
    v = v + swap_core(v)
    v = v + lax.ppermute(v, X, [(0, 1), (1, 0), (2, 3), (3, 2)])
    return v + lax.ppermute(v, X, [(0, 3), (3, 0), (1, 2), (2, 1)])


def call(kernel, out_shape, limit, *args, scratch=(), specs=None):
    return pl.pallas_call(
        kernel,
        in_specs=specs or [WHOLE] * len(args),
        out_specs=[WHOLE] * len(out_shape),
        out_shape=out_shape,
        scratch_shapes=list(scratch),
        compiler_params=pltpu.CompilerParams(vmem_limit_bytes=limit),
    )(*args)


def shape_of(*dims, dtype=bf16):
    return jax.ShapeDtypeStruct(dims, dtype)


def load_kernel(*refs):
    n = len(refs) // 2
    sems = refs[-1]
    copies = [pltpu.make_async_copy(refs[i], refs[n + i], sems.at[i]) for i in range(n)]
    for c in copies:
        c.start()
    for c in copies:
        c.wait()


def load(*weights):
    weights = [pltpu.with_memory_space_constraint(w, pltpu.HBM) for w in weights]
    return call(
        load_kernel,
        [pltpu.VMEM(w.shape, w.dtype) for w in weights],
        2 * MIB,
        *weights,
        specs=[HBM] * len(weights),
        scratch=[pltpu.SemaphoreType.DMA((len(weights),))],
    )


OVER_ROWS = (((0,), (0,)), ((), ()))


def pick(rows, cols, which, target):
    s = lax.broadcasted_iota(jnp.int32, (rows, cols), 0)
    slot = (s // 8) * 4 + s % 4
    hit = jnp.where((s // 4) % 2 == which, slot, -1) == target
    return jnp.where(hit, 1.0, 0.0).astype(bf16)


def mark_kernel(src, out):
    out[...] = src[...]


def positions(ids, experts):
    n = ids.shape[1]
    onehot = jnp.where(lax.broadcasted_iota(jnp.int32, (experts, n), 0) == ids, 1.0, 0.0)
    row = lax.broadcasted_iota(jnp.int32, (n, n), 0)
    col = lax.broadcasted_iota(jnp.int32, (n, n), 1)
    before = jnp.where(row < col, 1.0, 0.0).astype(bf16)
    earlier = jnp.dot(onehot.astype(bf16), before, preferred_element_type=f32)
    slot = jnp.sum(earlier * onehot, axis=0, keepdims=True).astype(jnp.int32)
    return ids * (n // experts) + slot


def pack_kernel(tokens, ids, sending, *, experts):
    micros, n, width = tokens.shape
    places = [pick(2 * n, n, m, positions(ids[m : m + 1, :], experts)) for m in range(micros)]
    for lo in range(0, width, 1024):
        at = slice(lo, lo + 1024)
        out = jnp.dot(places[0], tokens[0, :, at], preferred_element_type=f32)
        out = out + jnp.dot(places[1], tokens[1, :, at], preferred_element_type=f32)
        sending[:, at] = out.astype(bf16)
    ones = jnp.ones((n, STAT), bf16)
    fill = jnp.dot(places[0], ones, preferred_element_type=f32)
    fill = fill + jnp.dot(places[1], ones, preferred_element_type=f32)
    sending[:, width:] = fill.astype(bf16)


def pack(tokens, ids, experts):
    micros, n, width = tokens.shape
    return call(
        functools.partial(pack_kernel, experts=experts),
        [shape_of(micros * n, width + STAT)],
        8 * MIB,
        tokens,
        ids,
    )[0]


def split_kernel(arrived, *outs):
    *mine, counts = outs
    n, width = mine[0].shape
    rows = arrived.shape[0]
    for m, out in enumerate(mine):
        take = pick(rows, n, m, lax.broadcasted_iota(jnp.int32, (rows, n), 1))
        for lo in range(0, width, 1024):
            at = slice(lo, lo + 1024)
            out[:, at] = lax.dot_general(
                take, arrived[:, at], OVER_ROWS, preferred_element_type=f32
            ).astype(bf16)
    fill = arrived[:, width:].astype(f32)
    s = lax.broadcasted_iota(jnp.int32, fill.shape, 0)
    for m in range(len(mine)):
        count = jnp.sum(jnp.where((s // 4) % 2 == m, fill, 0.0), axis=0, keepdims=True)
        counts[m * 8 : m * 8 + 8, :] = jnp.broadcast_to(count, (8, STAT))


def split(arrived, micros, width):
    n = arrived.shape[0] // micros
    *mine, counts = call(
        split_kernel,
        [shape_of(n, width)] * micros + [shape_of(8 * micros, STAT, dtype=f32)],
        8 * MIB,
        arrived,
    )
    return mine, counts


def silu_mul(g, u):
    return (g / (1.0 + jnp.exp(-g)) * u).astype(bf16)


def gate_up_kernel(*refs, groups, keep):
    parts = refs[:groups]
    wg, wu = refs[groups : groups + 2]
    outs = refs[groups + 2 : -1]
    x = refs[-1]
    rows = parts[0].shape[0]
    for i, part in enumerate(parts):
        x[i * rows : (i + 1) * rows, :] = part[...]
    for lo in range(0, wg.shape[2], 128):
        at = slice(lo, lo + 128)
        w = jnp.concatenate([wg[0, :, at], wu[0, :, at]], axis=1)
        both = jnp.dot(x[...], w, preferred_element_type=f32)
        g = both[:, :128]
        u = both[:, 128:]
        if keep:
            outs[0][:, at] = g
            outs[1][:, at] = u
        else:
            outs[0][:, at] = silu_mul(g, u)


def gate_up(parts, w_gate, w_up, keep):
    rows, k = parts[0].shape
    dims = (len(parts) * rows, w_gate.shape[2])
    return call(
        functools.partial(gate_up_kernel, groups=len(parts), keep=keep),
        [shape_of(*dims, dtype=f32)] * 2 if keep else [shape_of(*dims)],
        14 * MIB,
        *parts,
        w_gate,
        w_up,
        scratch=[pltpu.VMEM((dims[0], k), bf16)],
    )


def clip_of(sumsq, count, width):
    return jnp.minimum(1.0, clip_target / jnp.sqrt((sumsq + width) / (width * (count + 1.0))))


def down_kernel(*refs, groups, keep):
    if keep:
        clip = clip_of(refs[0][:1, :1], refs[0][:1, 1:2], refs[-2].shape[1])
        parts = refs[1 : 1 + 2 * groups]
        sizes = [parts[2 * i].shape[0] // 2 for i in range(groups)]
    else:
        parts = refs[:groups]
        sizes = [p.shape[0] // 2 for p in parts]
    w, *owns, oth, h = refs[int(keep) + len(parts) :]
    n = owns[0].shape[0]
    rows = oth.shape[0]
    at = 0
    for i, size in enumerate(sizes):
        for side in range(2):
            src = slice(side * size, (side + 1) * size)
            dst = slice(side * rows + at, side * rows + at + size)
            if keep:
                h[dst, :] = silu_mul(clip * parts[2 * i][src, :], clip * parts[2 * i + 1][src, :])
            else:
                h[dst, :] = parts[i][src, :]
        at += size
    tile = 512

    def step(i, carry):
        cols = pl.ds(pl.multiple_of(i * tile, tile), tile)
        y = jnp.dot(h[...], w[0, :, cols], preferred_element_type=f32)
        for j, own in enumerate(owns):
            own[:, cols] = y[j * n : (j + 1) * n]
        oth[:, cols] = y[rows:].astype(oth.dtype)
        return carry

    steps = w.shape[2] // tile
    lax.fori_loop(0, steps, step, 0, unroll=steps if rows == n else 4)


def down(groups, w_down, n, stats):
    keep = stats is not None
    rows = sum(g[0].shape[0] for g in groups) // 2
    k, width = w_down.shape[1:]
    args = [a for g in groups for a in g]
    if keep:
        args = [stats] + args
    return call(
        functools.partial(down_kernel, groups=len(groups), keep=keep),
        [shape_of(n, width, dtype=f32)] * (rows // n) + [shape_of(rows, width)],
        12 * MIB,
        *args,
        w_down,
        scratch=[pltpu.VMEM((2 * rows, k), bf16)],
    )


def finish_kernel(own, other, near_a, near_b, counts, *outs, micro, last):
    n, width = own.shape
    half = width // 2
    tile = 512
    rows = 2 * n
    places = [pick(rows, n, h, lax.broadcasted_iota(jnp.int32, (rows, n), 1)) for h in range(2)]

    def step(i, total):
        out = None
        for h in range(2):
            cols = pl.ds(pl.multiple_of(h * half + i * tile, tile), tile)
            fin = own[:, cols] + other[:n, cols].astype(f32)
            fin = fin + (near_a[:, cols].astype(f32) + near_b[:, cols].astype(f32))
            part = jnp.dot(places[h], fin.astype(bf16), preferred_element_type=f32)
            out = part if out is None else out + part
            sq = fin * fin
            for j in range(0, tile, STAT):
                total = total + sq[:, j : j + STAT]
        outs[0][:, pl.ds(pl.multiple_of(i * tile, tile), tile)] = out.astype(bf16)
        return total

    total = lax.fori_loop(0, half // tile, step, jnp.zeros((n, STAT), f32))
    total = jnp.sum(jnp.sum(total, axis=0, keepdims=True), axis=1, keepdims=True)
    count = counts[micro * 8 : micro * 8 + 1, :1]
    if last:
        total = jnp.broadcast_to(total, (rows, STAT))
        lane = lax.broadcasted_iota(jnp.int32, (rows, STAT), 1)
        high = total.astype(bf16).astype(f32)
        middle = (total - high).astype(bf16).astype(f32)
        low = total - high - middle
        stats = jnp.where(lane == 0, high, jnp.where(lane == 1, middle, low))
        stats = jnp.where(lane < 3, stats, jnp.where(lane == 3, count, 0.0))
        outs[0][:, half:] = stats.astype(bf16)
    else:
        lane = lax.broadcasted_iota(jnp.int32, (8, STAT), 1)
        total = jnp.broadcast_to(total, (8, STAT))
        outs[1][...] = jnp.where(lane == 0, total, jnp.where(lane == 1, count, 0.0))


def finish(own, other, near_a, near_b, counts, micro, last):
    n, width = own.shape
    half = width // 2
    if last:
        outs = [shape_of(2 * n, half + STAT)]
    else:
        outs = [shape_of(2 * n, half), shape_of(8, STAT, dtype=f32)]
    return call(
        functools.partial(finish_kernel, micro=micro, last=last),
        outs,
        10 * MIB,
        own,
        other,
        near_a,
        near_b,
        counts,
    )


def unpack_kernel(*refs, experts):
    *backs, ids, out = refs
    n, width = out.shape[1:]
    half = width // 2
    for m, back in enumerate(backs):
        position = positions(ids[m : m + 1, :], experts)
        for h in range(2):
            take = pick(2 * n, n, h, position)
            for lo in range(0, half, 1024):
                out[m, :, h * half + lo : h * half + lo + 1024] = lax.dot_general(
                    take, back[:, lo : lo + 1024], OVER_ROWS, preferred_element_type=f32
                ).astype(bf16)


def exchange(v):
    experts = lax.axis_size(PLANE)
    rows, width = v.shape
    out = lax.all_to_all(v.reshape(experts, rows // experts, width), PLANE, 0, 0, tiled=True)
    return out.reshape(rows, width)


def body(tokens, expert_of, w_gate, w_up, w_down):
    micros, n, width = tokens.shape
    experts = lax.axis_size(PLANE)
    tie = lax.optimization_barrier

    arrived = exchange(pack(tokens, expert_of, experts))
    mine, counts = split(arrived, micros, width)
    w_gate, w_up, w_down = load(w_gate, w_up, w_down)
    (counts,) = call(mark_kernel, [shape_of(*counts.shape, dtype=f32)], MIB, counts)

    def spread_near(m):
        a = along_x(mine[m], 1)
        b = along_x(mine[m], -1)
        o = swap_core(mine[m])
        own = gate_up([mine[m], o], w_gate, w_up, m > 0)
        return a, b, own

    def spread_far(m, a, b):
        far = along_x(a, 1)
        ao = swap_core(a)
        bo = swap_core(b)
        near = gate_up([a, b, ao, bo], w_gate, w_up, m > 0)
        return far, near

    def spread_last(m, far):
        return gate_up([far, swap_core(far)], w_gate, w_up, m > 0)

    def collect(m, own, near, far, stats, fill_in):
        mid, send_far = down([far], w_down, n, stats)
        mid = mid + swap_core(send_far).astype(f32)
        relay = along_x(mid.astype(bf16), 1)
        mine_o, a_o, b_o, send = down([own, near], w_down, n, stats)
        got = swap_core(send)
        to_a = (a_o + got[n : 2 * n].astype(f32)).astype(bf16)
        from_b = along_x(to_a, -1)
        got_b, relay = tie((got, relay))
        to_b = (b_o + got_b[2 * n :].astype(f32) + relay.astype(f32)).astype(bf16)
        from_a = along_x(to_b, 1)
        from_a, from_b, extra = fill_in(from_a, from_b)
        last = m + 1 == micros
        return finish(mine_o, got, from_a, from_b, counts, m, last), extra

    a0, b0, own0 = spread_near(0)
    far0, near0 = spread_far(0, a0, b0)
    mine[1], near0 = tie((mine[1], near0))
    a1, b1, own1 = spread_near(1)
    far0 = spread_last(0, far0)

    def gates_of_1(from_a, from_b):
        ao = swap_core(a1)
        bo = swap_core(b1)
        near1 = gate_up([a1, b1, ao, bo], w_gate, w_up, True)
        from_a, from_b, near1 = tie((from_a, from_b, near1))
        far1 = along_x(a1, 1)
        return from_a, from_b, (near1, far1)

    (out0, stats), (near1, far1) = collect(0, own0, near0, far0, None, gates_of_1)
    stats = line_sum(stats)
    far1 = spread_last(1, far1)

    def return_0(from_a, from_b):
        back = exchange(out0)
        from_a, from_b, back = tie((from_a, from_b, back))
        return from_a, from_b, back

    (out1,), back0 = collect(1, own1, near1, far1, stats, return_0)
    back1 = exchange(out1)
    got = line_sum(back1[:: 2 * n // experts, width // 2 :].astype(f32))
    scale = clip_of(got[:, 0] + got[:, 1] + got[:, 2], got[:, 3], width)
    (out,) = call(
        functools.partial(unpack_kernel, experts=experts),
        [shape_of(micros, n, width)],
        8 * MIB,
        back0,
        back1[:, : width // 2],
        expert_of,
    )
    return out, scale


def solution(mesh):
    finer = Mesh(
        mesh.devices.reshape(mesh.shape["dp"], 4, 4, 2), ("dp", "expert_0", "expert_1", "expert_2")
    )
    placed = (
        P(None, DP_EXPERT, None),
        P(None, DP_EXPERT),
        P(EXPERT, None, "dp"),
        P(EXPERT, None, "dp"),
        P(EXPERT, "dp", None),
    )
    return jax.shard_map(
        body,
        mesh=finer,
        in_specs=placed,
        out_specs=(P(None, DP_EXPERT, None), P()),
        check_vma=False,
    )
```

```python
import functools

import jax
import jax.numpy as jnp
from jax import lax
from jax.experimental import pallas as pl
from jax.experimental.pallas import tpu as pltpu
from jax.sharding import Mesh
from jax.sharding import PartitionSpec as P

X = "dp"
PLANE = ("expert_0", "expert_1")
CORE = "expert_2"
EXPERT = ("expert_0", "expert_1", "expert_2")
DP_EXPERT = ("dp", "expert_0", "expert_1", "expert_2")
STAT = 128
MIB = 1 << 20

clip_target = 2.0


WHOLE = pl.BlockSpec(memory_space=pltpu.VMEM)
HBM = pl.BlockSpec(memory_space=pltpu.HBM)
f32 = jnp.float32
bf16 = jnp.bfloat16


def along_x(v, sign):
    n = lax.axis_size(X)
    pairs = []
    for i in range(n):
        pairs.append((2 * i, 2 * ((i + sign) % n)))
        pairs.append((2 * i + 1, 2 * ((i - sign) % n) + 1))
    return lax.ppermute(v, (X, CORE), pairs)


def swap_core(v):
    return lax.ppermute(v, CORE, [(0, 1), (1, 0)])


def line_sum(v):
    v = v + swap_core(v)
    v = v + lax.ppermute(v, X, [(0, 1), (1, 0), (2, 3), (3, 2)])
    return v + lax.ppermute(v, X, [(0, 3), (3, 0), (1, 2), (2, 1)])


def call(kernel, out_shape, limit, *args, scratch=(), specs=None):
    return pl.pallas_call(
        kernel,
        in_specs=specs or [WHOLE] * len(args),
        out_specs=[WHOLE] * len(out_shape),
        out_shape=out_shape,
        scratch_shapes=list(scratch),
        compiler_params=pltpu.CompilerParams(vmem_limit_bytes=limit),
    )(*args)


def shape_of(*dims, dtype=bf16):
    return jax.ShapeDtypeStruct(dims, dtype)


def load_kernel(*refs):
    n = len(refs) // 2
    sems = refs[-1]
    copies = [pltpu.make_async_copy(refs[i], refs[n + i], sems.at[i]) for i in range(n)]
    for c in copies:
        c.start()
    for c in copies:
        c.wait()


def load(*weights):
    weights = [pltpu.with_memory_space_constraint(w, pltpu.HBM) for w in weights]
    return call(
        load_kernel,
        [pltpu.VMEM(w.shape, w.dtype) for w in weights],
        2 * MIB,
        *weights,
        specs=[HBM] * len(weights),
        scratch=[pltpu.SemaphoreType.DMA((len(weights),))],
    )


OVER_ROWS = (((0,), (0,)), ((), ()))


def pick(rows, cols, which, target):
    s = lax.broadcasted_iota(jnp.int32, (rows, cols), 0)
    slot = (s // 8) * 4 + s % 4
    hit = jnp.where((s // 4) % 2 == which, slot, -1) == target
    return jnp.where(hit, 1.0, 0.0).astype(bf16)


def mark_kernel(src, out):
    out[...] = src[...]


def positions(ids, experts):
    n = ids.shape[1]
    onehot = jnp.where(lax.broadcasted_iota(jnp.int32, (experts, n), 0) == ids, 1.0, 0.0)
    row = lax.broadcasted_iota(jnp.int32, (n, n), 0)
    col = lax.broadcasted_iota(jnp.int32, (n, n), 1)
    before = jnp.where(row < col, 1.0, 0.0).astype(bf16)
    earlier = jnp.dot(onehot.astype(bf16), before, preferred_element_type=f32)
    slot = jnp.sum(earlier * onehot, axis=0, keepdims=True).astype(jnp.int32)
    return ids * (n // experts) + slot


def pack_kernel(tokens, ids, sending, *, experts):
    micros, n, width = tokens.shape
    places = [pick(2 * n, n, m, positions(ids[m : m + 1, :], experts)) for m in range(micros)]
    for lo in range(0, width, 1024):
        at = slice(lo, lo + 1024)
        out = jnp.dot(places[0], tokens[0, :, at], preferred_element_type=f32)
        out = out + jnp.dot(places[1], tokens[1, :, at], preferred_element_type=f32)
        sending[:, at] = out.astype(bf16)
    ones = jnp.ones((n, STAT), bf16)
    fill = jnp.dot(places[0], ones, preferred_element_type=f32)
    fill = fill + jnp.dot(places[1], ones, preferred_element_type=f32)
    sending[:, width:] = fill.astype(bf16)


def pack(tokens, ids, experts):
    micros, n, width = tokens.shape
    return call(
        functools.partial(pack_kernel, experts=experts),
        [shape_of(micros * n, width + STAT)],
        8 * MIB,
        tokens,
        ids,
    )[0]


def split_kernel(arrived, *outs):
    *mine, counts = outs
    n, width = mine[0].shape
    rows = arrived.shape[0]
    for m, out in enumerate(mine):
        take = pick(rows, n, m, lax.broadcasted_iota(jnp.int32, (rows, n), 1))
        for lo in range(0, width, 1024):
            at = slice(lo, lo + 1024)
            out[:, at] = lax.dot_general(
                take, arrived[:, at], OVER_ROWS, preferred_element_type=f32
            ).astype(bf16)
    fill = arrived[:, width:].astype(f32)
    s = lax.broadcasted_iota(jnp.int32, fill.shape, 0)
    for m in range(len(mine)):
        count = jnp.sum(jnp.where((s // 4) % 2 == m, fill, 0.0), axis=0, keepdims=True)
        counts[m * 8 : m * 8 + 8, :] = jnp.broadcast_to(count, (8, STAT))


def split(arrived, micros, width):
    n = arrived.shape[0] // micros
    *mine, counts = call(
        split_kernel,
        [shape_of(n, width)] * micros + [shape_of(8 * micros, STAT, dtype=f32)],
        8 * MIB,
        arrived,
    )
    return mine, counts


def silu_mul(g, u):
    return (g / (1.0 + jnp.exp(-g)) * u).astype(bf16)


def gate_up_kernel(*refs, groups, keep):
    parts = refs[:groups]
    wg, wu = refs[groups : groups + 2]
    outs = refs[groups + 2 : -1]
    x = refs[-1]
    rows = parts[0].shape[0]
    for i, part in enumerate(parts):
        x[i * rows : (i + 1) * rows, :] = part[...]
    for lo in range(0, wg.shape[2], 128):
        at = slice(lo, lo + 128)
        w = jnp.concatenate([wg[0, :, at], wu[0, :, at]], axis=1)
        both = jnp.dot(x[...], w, preferred_element_type=f32)
        g = both[:, :128]
        u = both[:, 128:]
        if keep:
            outs[0][:, at] = g
            outs[1][:, at] = u
        else:
            outs[0][:, at] = silu_mul(g, u)


def gate_up(parts, w_gate, w_up, keep):
    rows, k = parts[0].shape
    dims = (len(parts) * rows, w_gate.shape[2])
    return call(
        functools.partial(gate_up_kernel, groups=len(parts), keep=keep),
        [shape_of(*dims, dtype=f32)] * 2 if keep else [shape_of(*dims)],
        14 * MIB,
        *parts,
        w_gate,
        w_up,
        scratch=[pltpu.VMEM((dims[0], k), bf16)],
    )


def clip_of(sumsq, count, width):
    return jnp.minimum(1.0, clip_target / jnp.sqrt((sumsq + width) / (width * (count + 1.0))))


def down_kernel(*refs, groups, keep):
    if keep:
        clip = clip_of(refs[0][:1, :1], refs[0][:1, 1:2], refs[-2].shape[1])
        parts = refs[1 : 1 + 2 * groups]
        sizes = [parts[2 * i].shape[0] // 2 for i in range(groups)]
    else:
        parts = refs[:groups]
        sizes = [p.shape[0] // 2 for p in parts]
    w, *owns, oth, h = refs[int(keep) + len(parts) :]
    n = owns[0].shape[0]
    rows = oth.shape[0]
    at = 0
    for i, size in enumerate(sizes):
        for side in range(2):
            src = slice(side * size, (side + 1) * size)
            dst = slice(side * rows + at, side * rows + at + size)
            if keep:
                h[dst, :] = silu_mul(clip * parts[2 * i][src, :], clip * parts[2 * i + 1][src, :])
            else:
                h[dst, :] = parts[i][src, :]
        at += size
    tile = 512

    def step(i, carry):
        cols = pl.ds(pl.multiple_of(i * tile, tile), tile)
        y = jnp.dot(h[...], w[0, :, cols], preferred_element_type=f32)
        for j, own in enumerate(owns):
            own[:, cols] = y[j * n : (j + 1) * n]
        oth[:, cols] = y[rows:].astype(oth.dtype)
        return carry

    steps = w.shape[2] // tile
    lax.fori_loop(0, steps, step, 0, unroll=steps if rows == n else 4)


def down(groups, w_down, n, stats):
    keep = stats is not None
    rows = sum(g[0].shape[0] for g in groups) // 2
    k, width = w_down.shape[1:]
    args = [a for g in groups for a in g]
    if keep:
        args = [stats] + args
    return call(
        functools.partial(down_kernel, groups=len(groups), keep=keep),
        [shape_of(n, width, dtype=f32)] * (rows // n) + [shape_of(rows, width)],
        12 * MIB,
        *args,
        w_down,
        scratch=[pltpu.VMEM((2 * rows, k), bf16)],
    )


def finish_kernel(own, other, near_a, near_b, counts, *outs, micro, last):
    n, width = own.shape
    half = width // 2
    tile = 512
    rows = 2 * n
    places = [pick(rows, n, h, lax.broadcasted_iota(jnp.int32, (rows, n), 1)) for h in range(2)]

    def step(i, total):
        out = None
        for h in range(2):
            cols = pl.ds(pl.multiple_of(h * half + i * tile, tile), tile)
            fin = own[:, cols] + other[:n, cols].astype(f32)
            fin = fin + (near_a[:, cols].astype(f32) + near_b[:, cols].astype(f32))
            part = jnp.dot(places[h], fin.astype(bf16), preferred_element_type=f32)
            out = part if out is None else out + part
            sq = fin * fin
            for j in range(0, tile, STAT):
                total = total + sq[:, j : j + STAT]
        outs[0][:, pl.ds(pl.multiple_of(i * tile, tile), tile)] = out.astype(bf16)
        return total

    total = lax.fori_loop(0, half // tile, step, jnp.zeros((n, STAT), f32))
    total = jnp.sum(jnp.sum(total, axis=0, keepdims=True), axis=1, keepdims=True)
    count = counts[micro * 8 : micro * 8 + 1, :1]
    if last:
        total = jnp.broadcast_to(total, (rows, STAT))
        lane = lax.broadcasted_iota(jnp.int32, (rows, STAT), 1)
        high = total.astype(bf16).astype(f32)
        middle = (total - high).astype(bf16).astype(f32)
        low = total - high - middle
        stats = jnp.where(lane == 0, high, jnp.where(lane == 1, middle, low))
        stats = jnp.where(lane < 3, stats, jnp.where(lane == 3, count, 0.0))
        outs[0][:, half:] = stats.astype(bf16)
    else:
        lane = lax.broadcasted_iota(jnp.int32, (8, STAT), 1)
        total = jnp.broadcast_to(total, (8, STAT))
        outs[1][...] = jnp.where(lane == 0, total, jnp.where(lane == 1, count, 0.0))


def finish(own, other, near_a, near_b, counts, micro, last):
    n, width = own.shape
    half = width // 2
    if last:
        outs = [shape_of(2 * n, half + STAT)]
    else:
        outs = [shape_of(2 * n, half), shape_of(8, STAT, dtype=f32)]
    return call(
        functools.partial(finish_kernel, micro=micro, last=last),
        outs,
        10 * MIB,
        own,
        other,
        near_a,
        near_b,
        counts,
    )


def unpack_kernel(*refs, experts):
    *backs, ids, out = refs
    n, width = out.shape[1:]
    half = width // 2
    for m, back in enumerate(backs):
        position = positions(ids[m : m + 1, :], experts)
        for h in range(2):
            take = pick(2 * n, n, h, position)
            for lo in range(0, half, 1024):
                out[m, :, h * half + lo : h * half + lo + 1024] = lax.dot_general(
                    take, back[:, lo : lo + 1024], OVER_ROWS, preferred_element_type=f32
                ).astype(bf16)


def exchange(v):
    experts = lax.axis_size(PLANE)
    rows, width = v.shape
    out = lax.all_to_all(v.reshape(experts, rows // experts, width), PLANE, 0, 0, tiled=True)
    return out.reshape(rows, width)


def body(tokens, expert_of, w_gate, w_up, w_down):
    micros, n, width = tokens.shape
    experts = lax.axis_size(PLANE)
    tie = lax.optimization_barrier

    arrived = exchange(pack(tokens, expert_of, experts))
    mine, counts = split(arrived, micros, width)
    w_gate, w_up, w_down = load(w_gate, w_up, w_down)
    (counts,) = call(mark_kernel, [shape_of(*counts.shape, dtype=f32)], MIB, counts)

    def spread_near(m):
        a = along_x(mine[m], 1)
        b = along_x(mine[m], -1)
        o = swap_core(mine[m])
        own = gate_up([mine[m], o], w_gate, w_up, m > 0)
        return a, b, own

    def spread_far(m, a, b):
        far = along_x(a, 1)
        ao = swap_core(a)
        bo = swap_core(b)
        near = gate_up([a, b, ao, bo], w_gate, w_up, m > 0)
        return far, near

    def spread_last(m, far):
        return gate_up([far, swap_core(far)], w_gate, w_up, m > 0)

    def collect(m, own, near, far, stats, fill_in):
        mid, send_far = down([far], w_down, n, stats)
        mid = mid + swap_core(send_far).astype(f32)
        relay = along_x(mid.astype(bf16), 1)
        a_o, b_o, send = down([near], w_down, n, stats)
        got = swap_core(send)
        to_a = (a_o + got[:n].astype(f32)).astype(bf16)
        from_b = along_x(to_a, -1)
        got_b, relay = tie((got, relay))
        to_b = (b_o + got_b[n:].astype(f32) + relay.astype(f32)).astype(bf16)
        from_a = along_x(to_b, 1)
        mine_o, send = down([own], w_down, n, stats)
        got = swap_core(send)
        from_a, from_b, extra = fill_in(from_a, from_b)
        last = m + 1 == micros
        return finish(mine_o, got, from_a, from_b, counts, m, last), extra

    a0, b0, own0 = spread_near(0)
    far0, near0 = spread_far(0, a0, b0)
    mine[1], near0 = tie((mine[1], near0))
    a1, b1, own1 = spread_near(1)
    far0 = spread_last(0, far0)

    def gates_of_1(from_a, from_b):
        ao = swap_core(a1)
        bo = swap_core(b1)
        near1 = gate_up([a1, b1, ao, bo], w_gate, w_up, True)
        from_a, from_b, near1 = tie((from_a, from_b, near1))
        far1 = along_x(a1, 1)
        return from_a, from_b, (near1, far1)

    (out0, stats), (near1, far1) = collect(0, own0, near0, far0, None, gates_of_1)
    stats = line_sum(stats)
    far1 = spread_last(1, far1)

    def return_0(from_a, from_b):
        back = exchange(out0)
        from_a, from_b, back = tie((from_a, from_b, back))
        return from_a, from_b, back

    (out1,), back0 = collect(1, own1, near1, far1, stats, return_0)
    back1 = exchange(out1)
    got = line_sum(back1[:: 2 * n // experts, width // 2 :].astype(f32))
    scale = clip_of(got[:, 0] + got[:, 1] + got[:, 2], got[:, 3], width)
    (out,) = call(
        functools.partial(unpack_kernel, experts=experts),
        [shape_of(micros, n, width)],
        8 * MIB,
        back0,
        back1[:, : width // 2],
        expert_of,
    )
    return out, scale


def solution(mesh):
    finer = Mesh(
        mesh.devices.reshape(mesh.shape["dp"], 4, 4, 2), ("dp", "expert_0", "expert_1", "expert_2")
    )
    placed = (
        P(None, DP_EXPERT, None),
        P(None, DP_EXPERT),
        P(EXPERT, None, "dp"),
        P(EXPERT, None, "dp"),
        P(EXPERT, "dp", None),
    )
    return jax.shard_map(
        body,
        mesh=finer,
        in_specs=placed,
        out_specs=(P(None, DP_EXPERT, None), P()),
        check_vma=False,
    )
```

```python
import functools

import jax
import jax.numpy as jnp
from jax import lax
from jax.experimental import pallas as pl
from jax.experimental.pallas import tpu as pltpu
from jax.sharding import Mesh
from jax.sharding import PartitionSpec as P

X = "dp"
PLANE = ("expert_0", "expert_1")
CORE = "expert_2"
EXPERT = ("expert_0", "expert_1", "expert_2")
DP_EXPERT = ("dp", "expert_0", "expert_1", "expert_2")
STAT = 128
MIB = 1 << 20

clip_target = 2.0


WHOLE = pl.BlockSpec(memory_space=pltpu.VMEM)
HBM = pl.BlockSpec(memory_space=pltpu.HBM)
f32 = jnp.float32
bf16 = jnp.bfloat16


def along_x(v, sign):
    n = lax.axis_size(X)
    pairs = []
    for i in range(n):
        pairs.append((2 * i, 2 * ((i + sign) % n)))
        pairs.append((2 * i + 1, 2 * ((i - sign) % n) + 1))
    return lax.ppermute(v, (X, CORE), pairs)


def swap_core(v):
    return lax.ppermute(v, CORE, [(0, 1), (1, 0)])


def line_sum(v):
    near = swap_core(v)
    cores = [(x, c) for x in range(lax.axis_size(X)) for c in range(2)]
    across = lax.ppermute(v, (X, CORE), [(2 * x + c, 2 * (x ^ 1) + c) for x, c in cores])
    corner = lax.ppermute(v, (X, CORE), [(2 * x + c, 2 * (x ^ 1) + 1 - c) for x, c in cores])
    v = (v + near) + (across + corner)
    return v + lax.ppermute(v, X, [(0, 3), (3, 0), (1, 2), (2, 1)])


def call(kernel, out_shape, limit, *args, scratch=(), specs=None):
    return pl.pallas_call(
        kernel,
        in_specs=specs or [WHOLE] * len(args),
        out_specs=[WHOLE] * len(out_shape),
        out_shape=out_shape,
        scratch_shapes=list(scratch),
        compiler_params=pltpu.CompilerParams(vmem_limit_bytes=limit),
    )(*args)


def shape_of(*dims, dtype=bf16):
    return jax.ShapeDtypeStruct(dims, dtype)


def load_kernel(*refs):
    n = len(refs) // 2
    sems = refs[-1]
    copies = [pltpu.make_async_copy(refs[i], refs[n + i], sems.at[i]) for i in range(n)]
    for c in copies:
        c.start()
    for c in copies:
        c.wait()


def load(*weights):
    weights = [pltpu.with_memory_space_constraint(w, pltpu.HBM) for w in weights]
    return call(
        load_kernel,
        [pltpu.VMEM(w.shape, w.dtype) for w in weights],
        2 * MIB,
        *weights,
        specs=[HBM] * len(weights),
        scratch=[pltpu.SemaphoreType.DMA((len(weights),))],
    )


OVER_ROWS = (((0,), (0,)), ((), ()))


def pick(rows, cols, which, target):
    s = lax.broadcasted_iota(jnp.int32, (rows, cols), 0)
    slot = (s // 8) * 4 + s % 4
    hit = jnp.where((s // 4) % 2 == which, slot, -1) == target
    return jnp.where(hit, 1.0, 0.0).astype(bf16)


def mark_kernel(src, out):
    out[...] = src[...]


def positions(ids, experts):
    n = ids.shape[1]
    onehot = jnp.where(lax.broadcasted_iota(jnp.int32, (experts, n), 0) == ids, 1.0, 0.0)
    row = lax.broadcasted_iota(jnp.int32, (n, n), 0)
    col = lax.broadcasted_iota(jnp.int32, (n, n), 1)
    before = jnp.where(row < col, 1.0, 0.0).astype(bf16)
    earlier = jnp.dot(onehot.astype(bf16), before, preferred_element_type=f32)
    slot = jnp.sum(earlier * onehot, axis=0, keepdims=True).astype(jnp.int32)
    return ids * (n // experts) + slot


def pack_kernel(tokens, ids, sending, *, experts):
    micros, n, width = tokens.shape
    places = [pick(2 * n, n, m, positions(ids[m : m + 1, :], experts)) for m in range(micros)]
    for lo in range(0, width, 1024):
        at = slice(lo, lo + 1024)
        out = jnp.dot(places[0], tokens[0, :, at], preferred_element_type=f32)
        out = out + jnp.dot(places[1], tokens[1, :, at], preferred_element_type=f32)
        sending[:, at] = out.astype(bf16)
    ones = jnp.ones((n, STAT), bf16)
    fill = jnp.dot(places[0], ones, preferred_element_type=f32)
    fill = fill + jnp.dot(places[1], ones, preferred_element_type=f32)
    sending[:, width:] = fill.astype(bf16)


def pack(tokens, ids, experts):
    micros, n, width = tokens.shape
    return call(
        functools.partial(pack_kernel, experts=experts),
        [shape_of(micros * n, width + STAT)],
        8 * MIB,
        tokens,
        ids,
    )[0]


def split_kernel(arrived, *outs):
    *mine, counts = outs
    n, width = mine[0].shape
    rows = arrived.shape[0]
    for m, out in enumerate(mine):
        take = pick(rows, n, m, lax.broadcasted_iota(jnp.int32, (rows, n), 1))
        for lo in range(0, width, 1024):
            at = slice(lo, lo + 1024)
            out[:, at] = lax.dot_general(
                take, arrived[:, at], OVER_ROWS, preferred_element_type=f32
            ).astype(bf16)
    fill = arrived[:, width:].astype(f32)
    s = lax.broadcasted_iota(jnp.int32, fill.shape, 0)
    for m in range(len(mine)):
        count = jnp.sum(jnp.where((s // 4) % 2 == m, fill, 0.0), axis=0, keepdims=True)
        counts[m * 8 : m * 8 + 8, :] = jnp.broadcast_to(count, (8, STAT))


def split(arrived, micros, width):
    n = arrived.shape[0] // micros
    *mine, counts = call(
        split_kernel,
        [shape_of(n, width)] * micros + [shape_of(8 * micros, STAT, dtype=f32)],
        8 * MIB,
        arrived,
    )
    return mine, counts


def silu_mul(g, u):
    return (g / (1.0 + jnp.exp(-g)) * u).astype(bf16)


def gate_up_kernel(*refs, groups, keep):
    parts = refs[:groups]
    wg, wu = refs[groups : groups + 2]
    outs = refs[groups + 2 : -1]
    x = refs[-1]
    rows = parts[0].shape[0]
    for i, part in enumerate(parts):
        x[i * rows : (i + 1) * rows, :] = part[...]
    for lo in range(0, wg.shape[2], 128):
        at = slice(lo, lo + 128)
        w = jnp.concatenate([wg[0, :, at], wu[0, :, at]], axis=1)
        both = jnp.dot(x[...], w, preferred_element_type=f32)
        g = both[:, :128]
        u = both[:, 128:]
        if keep:
            outs[0][:, at] = g
            outs[1][:, at] = u
        else:
            outs[0][:, at] = silu_mul(g, u)


def gate_up(parts, w_gate, w_up, keep):
    rows, k = parts[0].shape
    dims = (len(parts) * rows, w_gate.shape[2])
    return call(
        functools.partial(gate_up_kernel, groups=len(parts), keep=keep),
        [shape_of(*dims, dtype=f32)] * 2 if keep else [shape_of(*dims)],
        14 * MIB,
        *parts,
        w_gate,
        w_up,
        scratch=[pltpu.VMEM((dims[0], k), bf16)],
    )


def clip_of(sumsq, count, width):
    return jnp.minimum(1.0, clip_target / jnp.sqrt((sumsq + width) / (width * (count + 1.0))))


def down_kernel(*refs, groups, keep):
    if keep:
        clip = clip_of(refs[0][:1, :1], refs[0][:1, 1:2], refs[-2].shape[1])
        parts = refs[1 : 1 + 2 * groups]
        sizes = [parts[2 * i].shape[0] // 2 for i in range(groups)]
    else:
        parts = refs[:groups]
        sizes = [p.shape[0] // 2 for p in parts]
    w, *owns, oth, h = refs[int(keep) + len(parts) :]
    n = owns[0].shape[0]
    rows = oth.shape[0]
    at = 0
    for i, size in enumerate(sizes):
        for side in range(2):
            src = slice(side * size, (side + 1) * size)
            dst = slice(side * rows + at, side * rows + at + size)
            if keep:
                h[dst, :] = silu_mul(clip * parts[2 * i][src, :], clip * parts[2 * i + 1][src, :])
            else:
                h[dst, :] = parts[i][src, :]
        at += size
    tile = 512

    def step(i, carry):
        cols = pl.ds(pl.multiple_of(i * tile, tile), tile)
        y = jnp.dot(h[...], w[0, :, cols], preferred_element_type=f32)
        for j, own in enumerate(owns):
            own[:, cols] = y[j * n : (j + 1) * n]
        oth[:, cols] = y[rows:].astype(oth.dtype)
        return carry

    steps = w.shape[2] // tile
    lax.fori_loop(0, steps, step, 0, unroll=steps if rows == n else 4)


def down(groups, w_down, n, stats):
    keep = stats is not None
    rows = sum(g[0].shape[0] for g in groups) // 2
    k, width = w_down.shape[1:]
    args = [a for g in groups for a in g]
    if keep:
        args = [stats] + args
    return call(
        functools.partial(down_kernel, groups=len(groups), keep=keep),
        [shape_of(n, width, dtype=f32)] * (rows // n) + [shape_of(rows, width)],
        12 * MIB,
        *args,
        w_down,
        scratch=[pltpu.VMEM((2 * rows, k), bf16)],
    )


def finish_kernel(own, other, near_a, near_b, counts, *outs, micro, last):
    n, width = own.shape
    half = width // 2
    tile = 512
    rows = 2 * n
    places = [pick(rows, n, h, lax.broadcasted_iota(jnp.int32, (rows, n), 1)) for h in range(2)]

    def step(i, total):
        out = None
        for h in range(2):
            cols = pl.ds(pl.multiple_of(h * half + i * tile, tile), tile)
            fin = own[:, cols] + other[:n, cols].astype(f32)
            fin = fin + (near_a[:, cols].astype(f32) + near_b[:, cols].astype(f32))
            part = jnp.dot(places[h], fin.astype(bf16), preferred_element_type=f32)
            out = part if out is None else out + part
            sq = fin * fin
            for j in range(0, tile, STAT):
                total = total + sq[:, j : j + STAT]
        outs[0][:, pl.ds(pl.multiple_of(i * tile, tile), tile)] = out.astype(bf16)
        return total

    total = lax.fori_loop(0, half // tile, step, jnp.zeros((n, STAT), f32))
    total = jnp.sum(jnp.sum(total, axis=0, keepdims=True), axis=1, keepdims=True)
    count = counts[micro * 8 : micro * 8 + 1, :1]
    if last:
        total = jnp.broadcast_to(total, (rows, STAT))
        lane = lax.broadcasted_iota(jnp.int32, (rows, STAT), 1)
        high = total.astype(bf16).astype(f32)
        middle = (total - high).astype(bf16).astype(f32)
        low = total - high - middle
        stats = jnp.where(lane == 0, high, jnp.where(lane == 1, middle, low))
        stats = jnp.where(lane < 3, stats, jnp.where(lane == 3, count, 0.0))
        outs[0][:, half:] = stats.astype(bf16)
    else:
        lane = lax.broadcasted_iota(jnp.int32, (8, STAT), 1)
        total = jnp.broadcast_to(total, (8, STAT))
        outs[1][...] = jnp.where(lane == 0, total, jnp.where(lane == 1, count, 0.0))


def finish(own, other, near_a, near_b, counts, micro, last):
    n, width = own.shape
    half = width // 2
    if last:
        outs = [shape_of(2 * n, half + STAT)]
    else:
        outs = [shape_of(2 * n, half), shape_of(8, STAT, dtype=f32)]
    return call(
        functools.partial(finish_kernel, micro=micro, last=last),
        outs,
        10 * MIB,
        own,
        other,
        near_a,
        near_b,
        counts,
    )


def unpack_kernel(*refs, experts):
    *backs, ids, out = refs
    n, width = out.shape[1:]
    half = width // 2
    for m, back in enumerate(backs):
        position = positions(ids[m : m + 1, :], experts)
        for h in range(2):
            take = pick(2 * n, n, h, position)
            for lo in range(0, half, 1024):
                out[m, :, h * half + lo : h * half + lo + 1024] = lax.dot_general(
                    take, back[:, lo : lo + 1024], OVER_ROWS, preferred_element_type=f32
                ).astype(bf16)


def exchange(v):
    experts = lax.axis_size(PLANE)
    rows, width = v.shape
    out = lax.all_to_all(v.reshape(experts, rows // experts, width), PLANE, 0, 0, tiled=True)
    return out.reshape(rows, width)


def body(tokens, expert_of, w_gate, w_up, w_down):
    micros, n, width = tokens.shape
    experts = lax.axis_size(PLANE)
    tie = lax.optimization_barrier

    arrived = exchange(pack(tokens, expert_of, experts))
    mine, counts = split(arrived, micros, width)
    w_gate, w_up, w_down = load(w_gate, w_up, w_down)
    (counts,) = call(mark_kernel, [shape_of(*counts.shape, dtype=f32)], MIB, counts)

    def spread_near(m):
        a = along_x(mine[m], 1)
        b = along_x(mine[m], -1)
        o = swap_core(mine[m])
        own = gate_up([mine[m], o], w_gate, w_up, m > 0)
        return a, b, own

    def spread_far(m, a, b):
        far = along_x(a, 1)
        ao = swap_core(a)
        bo = swap_core(b)
        near = gate_up([a, b, ao, bo], w_gate, w_up, m > 0)
        return far, near

    def spread_last(m, far):
        return gate_up([far, swap_core(far)], w_gate, w_up, m > 0)

    def collect(m, own, near, far, stats, fill_in):
        mid, send_far = down([far], w_down, n, stats)
        mid = mid + swap_core(send_far).astype(f32)
        relay = along_x(mid.astype(bf16), 1)
        a_o, b_o, send = down([near], w_down, n, stats)
        got = swap_core(send)
        to_a = (a_o + got[:n].astype(f32)).astype(bf16)
        from_b = along_x(to_a, -1)
        got_b, relay = tie((got, relay))
        to_b = (b_o + got_b[n:].astype(f32) + relay.astype(f32)).astype(bf16)
        from_a = along_x(to_b, 1)
        mine_o, send = down([own], w_down, n, stats)
        got = swap_core(send)
        from_a, from_b, extra = fill_in(from_a, from_b)
        last = m + 1 == micros
        return finish(mine_o, got, from_a, from_b, counts, m, last), extra

    a0, b0, own0 = spread_near(0)
    far0, near0 = spread_far(0, a0, b0)
    mine[1], near0 = tie((mine[1], near0))
    a1, b1, own1 = spread_near(1)
    far0 = spread_last(0, far0)

    def gates_of_1(from_a, from_b):
        ao = swap_core(a1)
        bo = swap_core(b1)
        near1 = gate_up([a1, b1, ao, bo], w_gate, w_up, True)
        from_a, from_b, near1 = tie((from_a, from_b, near1))
        far1 = along_x(a1, 1)
        return from_a, from_b, (near1, far1)

    (out0, stats), (near1, far1) = collect(0, own0, near0, far0, None, gates_of_1)
    stats = line_sum(stats)
    far1 = spread_last(1, far1)

    def return_0(from_a, from_b):
        back = exchange(out0)
        from_a, from_b, back = tie((from_a, from_b, back))
        return from_a, from_b, back

    (out1,), back0 = collect(1, own1, near1, far1, stats, return_0)
    back1 = exchange(out1)
    got = line_sum(back1[:: 2 * n // experts, width // 2 :].astype(f32))
    scale = clip_of(got[:, 0] + got[:, 1] + got[:, 2], got[:, 3], width)
    (out,) = call(
        functools.partial(unpack_kernel, experts=experts),
        [shape_of(micros, n, width)],
        8 * MIB,
        back0,
        back1[:, : width // 2],
        expert_of,
    )
    return out, scale


def solution(mesh):
    finer = Mesh(
        mesh.devices.reshape(mesh.shape["dp"], 4, 4, 2), ("dp", "expert_0", "expert_1", "expert_2")
    )
    placed = (
        P(None, DP_EXPERT, None),
        P(None, DP_EXPERT),
        P(EXPERT, None, "dp"),
        P(EXPERT, None, "dp"),
        P(EXPERT, "dp", None),
    )
    return jax.shard_map(
        body,
        mesh=finer,
        in_specs=placed,
        out_specs=(P(None, DP_EXPERT, None), P()),
        check_vma=False,
    )
```
